32 devices in a mesh: gx: 8 (over y, x, core), yz: 4 (over z).
Axes of the slice: x: 2, y: 2, z: 4, core: 2. Of those that a mesh axis runs over, the one named last changes fastest.
Arguments:
- spectra: bfloat16 [2, 20, 640, 16, 512], P(None, None, None, 'gx', 'yz'), may hold values from -6 to 6
- kernel_mesh: float32 [20], replicated, may hold values from 0.02 to 6, as said below
- density: float32 [640, 16, 512], P('gx', None, 'yz'), may hold values from 0.05 to 1
- local_wave: float32 [640, 16, 512], P('gx', None, 'yz'), may hold values from 0.15 to 4.8
- wave_density: float32 [640, 16, 512], P('gx', None, 'yz'), may hold values from -1.2 to 1.2
- wave_gradient: float32 [3, 640, 16, 512], P(None, 'gx', None, 'yz'), may hold values from -0.6 to 0.6
Outputs:
- potential: float32 [640, 16, 512], P('gx', None, 'yz')
The draws below stay inside these ranges and needn't reach their ends.
Inputs may be any that keep to these rules, and one draw needn't show every extreme that they name: `kernel_mesh`: strictly increasing; entry 0 is at most 0.1 and entry 19 at least 5.0.
All inputs are finite; a program needn't handle non-finite values.
Results may differ from the reference program's by a relative error of at most 0.0033.
Values sent between devices are 32-bit elements.
A program may use at most 192 MiB of HBM per device.

```python
import math
import jax
import jax.numpy as jnp
from jax import lax

NX = 640
COMP = 20
NY = 16
NZ = 512


def draw_kernel_mesh(key, part):
    first_key, last_key, step_key = jax.random.split(key, 3)
    first_point = jax.random.uniform(first_key, (), jnp.float32, 0.02, 0.1)
    last_point = jax.random.uniform(last_key, (), jnp.float32, 5.05, 6.0)
    logs = jax.random.uniform(step_key, (COMP - 1,), jnp.float32, math.log(0.5), math.log(2.0))
    steps_raw = jnp.exp(logs)
    steps_scaled = steps_raw / jnp.sum(steps_raw) * (last_point - first_point)
    return jnp.concatenate([first_point[None], first_point + jnp.cumsum(steps_scaled)])


def steps_of(own_key, shape, shards, low, largest):
    loudness = 1.0
    for position, blocks in shards:
        heights = jax.random.uniform(jax.random.fold_in(jax.random.fold_in(own_key, 6), position), (blocks,), jnp.float32, low / len(shards), largest / len(shards))
        loudness = loudness * jnp.repeat(jnp.exp(heights), shape[position] // blocks).reshape((-1,) + (1,) * (len(shape) - 1 - position))
    return loudness


def centred(own_key, dims, width, most, cuts=(), held_as=jnp.bfloat16):
    array = width * jax.random.normal(own_key, dims, jnp.float32)
    if cuts:
        array = array * steps_of(own_key, dims, cuts, -0.22, 0.18)
    return jnp.clip(array, -most, most).astype(held_as)


def setup_inputs(seed: int = 0) -> dict:
    seeds = jax.random.split(jax.random.key(seed), 7)
    return {
        "spectra": centred(seeds[0], (2, COMP, NX, NY, NZ), 1.0, 6.0, ((3, 8), (4, 4))),
        "kernel_mesh": draw_kernel_mesh(jax.random.fold_in(seeds[6], 71), 0),
        "density": jnp.clip(jnp.exp(math.log(1.0) - 2.9957323 * jax.random.uniform(seeds[2], (NX, NY, NZ), jnp.float32) ** steps_of(seeds[2], (NX, NY, NZ), ((0, 8), (2, 4)), -0.2, 0.2)), 0.05, 1.0),
        "local_wave": jnp.clip(0.15 + 4.65 * jax.random.uniform(seeds[3], (NX, NY, NZ), jnp.float32) ** steps_of(seeds[3], (NX, NY, NZ), ((0, 8), (2, 4)), -0.2, 0.2), 0.15, 4.8),
        "wave_density": centred(seeds[4], (NX, NY, NZ), 0.2, 1.2, ((0, 8), (2, 4)), jnp.float32),
        "wave_gradient": centred(seeds[5], (3, NX, NY, NZ), 0.1, 0.6, ((1, 8), (3, 4)), jnp.float32),
    }


def dft_tables(length):
    rows_index = lax.broadcasted_iota(jnp.int32, (length, length), 0)
    cols_index = lax.broadcasted_iota(jnp.int32, (length, length), 1)
    phases = rows_index * cols_index % length
    angles = phases.astype(jnp.float32) * (2.0 * math.pi / length)
    return jnp.stack([jnp.cos(angles), -jnp.sin(angles)]).astype(jnp.bfloat16)

def spline_second(kernel_mesh):
    points = kernel_mesh.shape[0]
    spacing = kernel_mesh[1:] - kernel_mesh[:-1]
    identity = jnp.eye(points, dtype=jnp.float32)
    right_side = (identity[2:] - identity[1:-1]) / spacing[1:, None] - (identity[1:-1] - identity[:-2]) / spacing[:-1, None]
    zero_entry = jnp.zeros((1,), jnp.float32)
    lower_band = jnp.concatenate([zero_entry, spacing[1:-1] / 6.0])
    main_band = (spacing[:-1] + spacing[1:]) / 3.0
    upper_band = jnp.concatenate([spacing[1:-1] / 6.0, zero_entry])
    interior = lax.linalg.tridiagonal_solve(lower_band, main_band, upper_band, right_side)
    border = jnp.zeros((1, points), jnp.float32)
    return jnp.concatenate([border, interior, border])

def basis_terms(weight_a, weight_b, span_width, lower_hot, upper_hot, second_lower, second_upper):
    basis_value = weight_a * lower_hot + weight_b * upper_hot + (weight_a * weight_a * weight_a - weight_a) * span_width * span_width / 6.0 * second_lower + (weight_b * weight_b * weight_b - weight_b) * span_width * span_width / 6.0 * second_upper
    basis_slope = (upper_hot - lower_hot) / span_width - (3.0 * weight_a * weight_a - 1.0) * span_width / 6.0 * second_lower + (3.0 * weight_b * weight_b - 1.0) * span_width / 6.0 * second_upper
    return (basis_value, basis_slope)

def reference(spectra, kernel_mesh, density, local_wave, wave_density, wave_gradient):
    tables = dft_tables(NX).astype(jnp.float32)
    second = spline_second(kernel_mesh)
    points = kernel_mesh.shape[0]
    interval = jnp.zeros(local_wave.shape, jnp.int32)
    for index in range(1, points - 1):
        interval = interval + (local_wave >= kernel_mesh[index]).astype(jnp.int32)
    lower_point = jnp.take(kernel_mesh, interval)
    finish_point = jnp.take(kernel_mesh, interval + 1)
    span_width = finish_point - lower_point
    weight_a = (finish_point - local_wave) / span_width
    weight_b = (local_wave - lower_point) / span_width

    def accumulate(carry, alpha):
        sum_value, sum_slope = carry
        spectrum = lax.dynamic_index_in_dim(spectra, alpha, 1, keepdims=False).astype(jnp.float32)
        summed = jnp.einsum('pkyz,pkx->xyz', spectrum, tables, precision=lax.Precision.HIGHEST)
        values = summed * NX ** (-0.5)
        lower_hot = (interval == alpha).astype(jnp.float32)
        upper_hot = (interval + 1 == alpha).astype(jnp.float32)
        column = lax.dynamic_index_in_dim(second, alpha, 1, keepdims=False)
        second_lower = jnp.take(column, interval)
        second_upper = jnp.take(column, interval + 1)
        basis_value, basis_slope = basis_terms(weight_a, weight_b, span_width, lower_hot, upper_hot, second_lower, second_upper)
        return ((sum_value + values * basis_value, sum_slope + values * basis_slope), None)
    blank_field = jnp.zeros(local_wave.shape, jnp.float32)
    (sum_value, sum_slope), unused = lax.scan(accumulate, (blank_field, blank_field), jnp.arange(points, dtype=jnp.int32))
    local_term = sum_value + density * wave_density * sum_slope
    grad_scale = density * sum_slope
    divergence = jnp.zeros(local_wave.shape, jnp.float32)
    for axis_index in range(3):
        flux = grad_scale * wave_gradient[axis_index]
        divergence = divergence + 0.5 * (jnp.roll(flux, -1, axis_index) - jnp.roll(flux, 1, axis_index))
    return local_term - divergence
```

```python
import functools
import math

import jax
import jax.numpy as jnp
import numpy as np
from jax import lax
from jax.experimental import pallas as pl
from jax.experimental.pallas import tpu as pltpu
from jax.sharding import PartitionSpec as P

SUB = 8


def split_tables(length, blocks, padded_rows):
    quarter = length // 4
    per_block = length // blocks // 4
    out = np.zeros((4, blocks, padded_rows, 2, quarter, 2), np.float32)
    k = np.arange(quarter)
    for r in range(4):
        m = np.arange(blocks * per_block).reshape(blocks, per_block)
        x = 4 * m + r
        phases = (x[..., None] * k) % length
        angles = phases.astype(np.float32) * np.float32(2.0 * math.pi / length)
        pair = np.stack([np.cos(angles), -np.sin(angles)], axis=2)
        for y in range(2):
            out[r, :, y : 2 * per_block : 2, :, :, y] = pair
    flat = out.reshape(4, blocks * padded_rows, 4 * quarter)
    return flat.astype(jnp.bfloat16)


def spline_coefficients(mesh_ref, coef_ref):
    points = mesh_ref.shape[0]
    ones = jnp.ones((SUB, 128), jnp.float32)
    node = [ones * mesh_ref[j] for j in range(points)]
    gap = [node[j + 1] - node[j] for j in range(points - 1)]
    carry = jnp.zeros((SUB, 128), jnp.float32)
    for j in range(points):
        coef_ref[0, j] = node[j]
        if j < points - 1:
            coef_ref[1, j] = 1.0 / gap[j]
        if 1 <= j < points - 1:
            pivot = 1.0 / (2.0 * (gap[j - 1] + gap[j]) - gap[j - 1] * carry)
            carry = gap[j] * pivot
            coef_ref[2, j] = pivot
            coef_ref[3, j] = gap[j - 1] * pivot
            coef_ref[4, j] = carry


def spline_sums(wave, value_of, coef_ref, points, scale):
    values = [value_of(j) for j in range(points)]
    forward = [None] * points
    slope_before = (values[1] - values[0]) * coef_ref[1, 0]
    for j in range(1, points - 1):
        slope_here = (values[j + 1] - values[j]) * coef_ref[1, j]
        term = (slope_here - slope_before) * coef_ref[2, j]
        if j > 1:
            term = term - coef_ref[3, j] * forward[j - 1]
        forward[j] = term
        slope_before = slope_here
    zero = jnp.zeros_like(wave)
    sixth = [zero] * points
    for j in range(points - 2, 0, -1):
        sixth[j] = forward[j] if j == points - 2 else forward[j] - coef_ref[4, j] * sixth[j + 1]
    picked = [values[0], values[1], sixth[0], sixth[1], coef_ref[0, 0], coef_ref[0, 1]]
    for j in range(1, points - 1):
        above = wave >= coef_ref[0, j]
        here = [values[j], values[j + 1], sixth[j], sixth[j + 1], coef_ref[0, j], coef_ref[0, j + 1]]
        picked = [jnp.where(above, new, old) for new, old in zip(here, picked)]
    value_low, value_high, sixth_low, sixth_high, low, high = picked
    width = high - low
    inverse = 1.0 / width
    a = (high - wave) * inverse
    b = (wave - low) * inverse
    square_a, square_b = a * a, b * b
    bent = ((square_a * a - a) * sixth_low + (square_b * b - b) * sixth_high) * (width * width)
    total = a * value_low + b * value_high + bent
    turn = ((3.0 * square_b - 1.0) * sixth_high - (3.0 * square_a - 1.0) * sixth_low) * width
    slope = (value_high - value_low) * inverse + turn
    return total * scale, slope * scale


def slab_kernel(blocks, padded, mesh_ref, spectra_ref, table_ref, wave_ref, out_ref, folded, comps, coef):
    step = pl.program_id(0)
    points = mesh_ref.shape[0]
    quarter_rows = spectra_ref.shape[3]
    chunk = 32
    for which in range(2):
        lanes = slice(which * 128, which * 128 + 128)

        @pl.loop(0, quarter_rows // chunk)
        def _(c):
            rows = pl.ds(pl.multiple_of(c * chunk, chunk), chunk)
            rows_im = pl.ds(pl.multiple_of(c * chunk + quarter_rows, chunk), chunk)
            re = [spectra_ref[0, which, s, rows, :].astype(jnp.float32) for s in range(4)]
            im = [spectra_ref[1, which, s, rows, :].astype(jnp.float32) for s in range(4)]
            a_re, b_re, c_re, d_re = re[0] + re[2], re[0] - re[2], re[1] + re[3], re[1] - re[3]
            a_im, b_im, c_im, d_im = im[0] + im[2], im[0] - im[2], im[1] + im[3], im[1] - im[3]
            parts = (
                (a_re + c_re, a_im + c_im),
                (b_re - d_im, b_im + d_re),
                (a_re - c_re, a_im - c_im),
                (b_re + d_im, b_im - d_re),
            )
            for r in range(4):
                folded[r, rows, lanes] = parts[r][0].astype(jnp.bfloat16)
                folded[r, rows_im, lanes] = parts[r][1].astype(jnp.bfloat16)

    for r in range(4):
        product = jnp.dot(table_ref[r], folded[r], preferred_element_type=jnp.float32)
        comps[2 * step, r] = product[:, :128]
        comps[2 * step + 1, r] = product[:, 128:]

    @pl.when(step == pl.num_programs(0) - 1)
    def _():
        spline_coefficients(mesh_ref, coef)
        scale = (quarter_rows * 2) ** (-0.5)

        @pl.loop(0, 4 * blocks)
        def _(index):
            block, r = index // 4, index % 4
            for v in range(padded // SUB):
                source = pl.ds(pl.multiple_of(block * padded + v * SUB, SUB), SUB)
                total, slope = spline_sums(
                    wave_ref[block, pl.ds(pl.multiple_of(r * padded + v * SUB, SUB), SUB), :],
                    lambda j: comps[j, r, source, :],
                    coef,
                    points,
                    scale,
                )
                out_ref[block, pl.ds(pl.multiple_of(r * padded + v * SUB, SUB), SUB), :] = total
                out_ref[block, pl.ds(pl.multiple_of((4 + r) * padded + v * SUB, SUB), SUB), :] = slope

        rows = quarter_rows * 4 // blocks // 4
        for block in range(blocks):
            before, after = (block - 1) % blocks, (block + 1) % blocks
            out_ref[block, 8 * padded : 8 * padded + 2, :] = out_ref[
                before, 7 * padded + rows - 2 : 7 * padded + rows, :
            ]
            out_ref[block, 8 * padded + 2 : 8 * padded + 4, :] = out_ref[
                after, 4 * padded : 4 * padded + 2, :
            ]
            out_ref[block, 8 * padded + 4 : 8 * padded + 8, :] = jnp.zeros((4, 128), jnp.float32)


def slab_sums(kernel_mesh, spectra, table, wave, blocks, padded):
    points = kernel_mesh.shape[0]
    _, comps, _, rows, lanes = spectra.shape
    out_rows = 8 * padded + 8
    return pl.pallas_call(
        functools.partial(slab_kernel, blocks, padded),
        grid=(comps // 2,),
        out_shape=jax.ShapeDtypeStruct((blocks, out_rows, lanes), jnp.float32),
        in_specs=[
            pl.BlockSpec(memory_space=pltpu.SMEM),
            pl.BlockSpec((2, 2, 4, rows, lanes), lambda i: (0, i, 0, 0, 0)),
            pl.BlockSpec(table.shape, lambda i: (0, 0, 0)),
            pl.BlockSpec(wave.shape, lambda i: (0, 0, 0)),
        ],
        out_specs=pl.BlockSpec((blocks, out_rows, lanes), lambda i: (0, 0, 0)),
        scratch_shapes=[
            pltpu.VMEM((4, 2 * rows, 2 * lanes), jnp.bfloat16),
            pltpu.VMEM((points, 4, blocks * padded, lanes), jnp.float32),
            pltpu.VMEM((5, points, SUB, 128), jnp.float32),
        ],
        compiler_params=pltpu.CompilerParams(
            dimension_semantics=("arbitrary",), vmem_limit_bytes=60 * 1024 * 1024
        ),
        cost_estimate=pl.CostEstimate(flops=2 * 10**10, bytes_accessed=2 * 10**7, transcendentals=0),
    )(kernel_mesh, spectra, table, wave)


def exchange_pairs(group, row):
    far = row < 4
    near = row % 4 < 2
    a, b, c, d = group
    a, c = jnp.where(far, a, pltpu.roll(c, 4, 0)), jnp.where(far, pltpu.roll(a, 4, 0), c)
    b, d = jnp.where(far, b, pltpu.roll(d, 4, 0)), jnp.where(far, pltpu.roll(b, 4, 0), d)
    a, b = jnp.where(near, a, pltpu.roll(b, 2, 0)), jnp.where(near, pltpu.roll(a, 6, 0), b)
    c, d = jnp.where(near, c, pltpu.roll(d, 2, 0)), jnp.where(near, pltpu.roll(c, 6, 0), d)
    return a, b, c, d


def domain_kernel(
    blocks,
    padded,
    sums_ref,
    density_ref,
    rate_ref,
    gradient_ref,
    edge_ref,
    out_ref,
    first,
    second,
    faces,
    arrived,
    send_sem,
    recv_sem,
):
    depth, height, lanes = density_ref.shape
    count = lax.axis_size("yz")
    me = lax.axis_index("yz")
    right, left = lax.rem(me + 1, count), lax.rem(me + count - 1, count)
    barrier = pltpu.get_barrier_semaphore()
    for neighbour in (left, right):
        pl.semaphore_signal(
            barrier, inc=1, device_id={"yz": neighbour}, device_id_type=pl.DeviceIdType.MESH
        )
    pl.semaphore_wait(barrier, 2)

    row = lax.broadcasted_iota(jnp.int32, (SUB, lanes), 0)
    lane = lax.broadcasted_iota(jnp.int32, (SUB, lanes), 1)
    per_class = depth // 4
    octets = height // SUB
    low_face = [jnp.zeros((SUB, lanes), jnp.float32)] * octets
    high_face = [jnp.zeros((SUB, lanes), jnp.float32)] * octets
    for octet in range(octets):
        ys = slice(octet * SUB, octet * SUB + SUB)
        for r in range(4):
            for quad in range(padded // SUB):
                totals = exchange_pairs(
                    [
                        sums_ref[4 * octet + j, r * padded + quad * SUB : r * padded + quad * SUB + SUB, :]
                        for j in range(4)
                    ],
                    row,
                )
                slopes = exchange_pairs(
                    [
                        sums_ref[
                            4 * octet + j, (4 + r) * padded + quad * SUB : (4 + r) * padded + quad * SUB + SUB, :
                        ]
                        for j in range(4)
                    ],
                    row,
                )
                for i in range(4):
                    if 4 * quad + i >= per_class:
                        continue
                    x = 4 * (4 * quad + i) + r
                    grad_scale = density_ref[x, ys, :] * slopes[i]
                    third = grad_scale * gradient_ref[2, x, ys, :]
                    onward = jnp.where(lane == lanes - 1, 0.0, pltpu.roll(third, lanes - 1, 1))
                    back = jnp.where(lane == 0, 0.0, pltpu.roll(third, 1, 1))
                    out_ref[x, ys, :] = totals[i] + rate_ref[x, ys, :] * grad_scale - 0.5 * (onward - back)
                    first[x + 1, ys, :] = grad_scale * gradient_ref[0, x, ys, :]
                    second[x, ys, :] = grad_scale * gradient_ref[1, x, ys, :]
                    low_face[octet] = jnp.where(lane == x, third[:, :1], low_face[octet])
                    high_face[octet] = jnp.where(lane == x, third[:, lanes - 1 :], high_face[octet])
        faces[0, ys, :] = low_face[octet]
        faces[1, ys, :] = high_face[octet]

    copies = []
    for side, neighbour in ((0, left), (1, right)):
        copy = pltpu.make_async_remote_copy(
            src_ref=faces.at[side],
            dst_ref=arrived.at[side],
            send_sem=send_sem.at[side],
            recv_sem=recv_sem.at[side],
            device_id={"yz": neighbour},
            device_id_type=pl.DeviceIdType.MESH,
        )
        copy.start()
        copies.append(copy)

    for octet in range(octets):
        ys = slice(octet * SUB, octet * SUB + SUB)
        for side, x in ((0, 0), (1, depth + 1)):
            edge = jnp.zeros((SUB, lanes), jnp.float32)
            for j in range(4):
                piece = sums_ref[4 * octet + j, 8 * padded : 8 * padded + SUB, :]
                shift = (2 * j - 2 * side) % SUB
                piece = pltpu.roll(piece, shift, 0) if shift else piece
                edge = jnp.where(row // 2 == j, piece, edge)
            first[x, ys, :] = edge * edge_ref[side, ys, :]

    rows_all = lax.broadcasted_iota(jnp.int32, (SUB, lanes), 0)

    @pl.loop(0, depth)
    def _(x):
        pieces = [second[x, o * SUB : o * SUB + SUB, :] for o in range(octets)]
        up = [pltpu.roll(p, SUB - 1, 0) for p in pieces]
        down = [pltpu.roll(p, 1, 0) for p in pieces]
        for o in range(octets):
            ys = slice(o * SUB, o * SUB + SUB)
            following = jnp.where(rows_all == SUB - 1, up[(o + 1) % octets], up[o])
            previous = jnp.where(rows_all == 0, down[o - 1], down[o])
            along = first[x + 2, ys, :] - first[x, ys, :]
            out_ref[x, ys, :] = out_ref[x, ys, :] - 0.5 * (along + (following - previous))

    for copy in copies:
        copy.wait()
    for o in range(octets):
        ys = slice(o * SUB, o * SUB + SUB)
        next_face, previous_face = arrived[0, ys, :], arrived[1, ys, :]
        for x in range(depth):
            edges = jnp.where(lane == lanes - 1, next_face[:, x : x + 1], 0.0) - jnp.where(
                lane == 0, previous_face[:, x : x + 1], 0.0
            )
            out_ref[x, ys, :] = out_ref[x, ys, :] - 0.5 * edges


def domain_result(sums, density, rate, gradient, edges, blocks, padded):
    depth, height, lanes = density.shape
    vmem = pl.BlockSpec(memory_space=pltpu.VMEM)
    return pl.pallas_call(
        functools.partial(domain_kernel, blocks, padded),
        out_shape=jax.ShapeDtypeStruct(density.shape, jnp.float32),
        in_specs=[vmem] * 5,
        out_specs=vmem,
        scratch_shapes=[
            pltpu.VMEM((depth + 2, height, lanes), jnp.float32),
            pltpu.VMEM((depth, height, lanes), jnp.float32),
            pltpu.VMEM((2, height, lanes), jnp.float32),
            pltpu.VMEM((2, height, lanes), jnp.float32),
            pltpu.SemaphoreType.DMA((2,)),
            pltpu.SemaphoreType.DMA((2,)),
        ],
        compiler_params=pltpu.CompilerParams(collective_id=0, has_side_effects=True),
    )(sums, density, rate, gradient, edges)


def solution(mesh):
    blocks = mesh.shape["gx"]

    def shards(spectra, kernel_mesh, density, local_wave, wave_density, wave_gradient):
        _, points, length, thin, lanes = spectra.shape
        depth, height, _ = density.shape
        per_class = depth // 4
        padded = -(-2 * per_class // SUB) * SUB
        table = jnp.asarray(split_tables(length, blocks, padded))
        forward = [(i, (i + 1) % blocks) for i in range(blocks)]
        backward = [(i, (i - 1) % blocks) for i in range(blocks)]
        product = density * wave_gradient[0]
        edges = jnp.stack(
            [
                lax.ppermute(product[-1], "gx", forward),
                lax.ppermute(product[0], "gx", backward),
            ]
        )
        wave = local_wave.reshape(per_class, 4, blocks, 2, lanes).transpose(2, 1, 0, 3, 4)
        wave = wave.reshape(blocks, 4, 2 * per_class, lanes)
        wave = lax.all_to_all(wave, "gx", split_axis=0, concat_axis=0, tiled=True)
        wave = jnp.pad(wave, ((0, 0), (0, 0), (0, padded - 2 * per_class), (0, 0)))
        wave = wave.reshape(blocks, 4 * padded, lanes)
        sums = slab_sums(
            kernel_mesh, spectra.reshape(2, points, 4, length // 2, lanes), table, wave, blocks, padded
        )
        sums = lax.all_to_all(sums, "gx", split_axis=0, concat_axis=0, tiled=True)
        return domain_result(sums, density, wave_density, wave_gradient, edges, blocks, padded)

    return jax.shard_map(
        shards,
        mesh=mesh,
        in_specs=(
            P(None, None, None, "gx", "yz"),
            P(),
            P("gx", None, "yz"),
            P("gx", None, "yz"),
            P("gx", None, "yz"),
            P(None, "gx", None, "yz"),
        ),
        out_specs=P("gx", None, "yz"),
        check_vma=False,
    )
```

```python
import functools
import math

import jax
import jax.numpy as jnp
import numpy as np
from jax import lax
from jax.experimental import pallas as pl
from jax.experimental.pallas import tpu as pltpu
from jax.sharding import PartitionSpec as P

SUB = 8


def split_tables(length, blocks, padded_rows):
    quarter = length // 4
    per_block = length // blocks // 4
    out = np.zeros((4, blocks, padded_rows, 2, quarter, 2), np.float32)
    k = np.arange(quarter)
    for r in range(4):
        m = np.arange(blocks * per_block).reshape(blocks, per_block)
        x = 4 * m + r
        phases = (x[..., None] * k) % length
        angles = phases.astype(np.float32) * np.float32(2.0 * math.pi / length)
        pair = np.stack([np.cos(angles), -np.sin(angles)], axis=2)
        for y in range(2):
            out[r, :, y : 2 * per_block : 2, :, :, y] = pair
    flat = out.reshape(4, blocks * padded_rows, 4 * quarter)
    return flat.astype(jnp.bfloat16)


def spline_coefficients(mesh_ref, coef_ref):
    points = mesh_ref.shape[0]
    ones = jnp.ones((SUB, 128), jnp.float32)
    node = [ones * mesh_ref[j] for j in range(points)]
    gap = [node[j + 1] - node[j] for j in range(points - 1)]
    carry = jnp.zeros((SUB, 128), jnp.float32)
    for j in range(points):
        coef_ref[0, j] = node[j]
        if j < points - 1:
            coef_ref[1, j] = 1.0 / gap[j]
        if 1 <= j < points - 1:
            pivot = 1.0 / (2.0 * (gap[j - 1] + gap[j]) - gap[j - 1] * carry)
            carry = gap[j] * pivot
            coef_ref[2, j] = pivot
            coef_ref[3, j] = gap[j - 1] * pivot
            coef_ref[4, j] = carry


def spline_sums(wave, value_of, coef_ref, points, scale):
    values = [value_of(j) for j in range(points)]
    forward = [None] * points
    slope_before = (values[1] - values[0]) * coef_ref[1, 0]
    for j in range(1, points - 1):
        slope_here = (values[j + 1] - values[j]) * coef_ref[1, j]
        term = (slope_here - slope_before) * coef_ref[2, j]
        if j > 1:
            term = term - coef_ref[3, j] * forward[j - 1]
        forward[j] = term
        slope_before = slope_here
    zero = jnp.zeros_like(wave)
    sixth = [zero] * points
    for j in range(points - 2, 0, -1):
        sixth[j] = forward[j] if j == points - 2 else forward[j] - coef_ref[4, j] * sixth[j + 1]
    picked = [values[0], values[1], sixth[0], sixth[1], coef_ref[0, 0], coef_ref[0, 1]]
    for j in range(1, points - 1):
        above = wave >= coef_ref[0, j]
        here = [values[j], values[j + 1], sixth[j], sixth[j + 1], coef_ref[0, j], coef_ref[0, j + 1]]
        picked = [jnp.where(above, new, old) for new, old in zip(here, picked)]
    value_low, value_high, sixth_low, sixth_high, low, high = picked
    width = high - low
    inverse = 1.0 / width
    a = (high - wave) * inverse
    b = (wave - low) * inverse
    square_a, square_b = a * a, b * b
    bent = ((square_a * a - a) * sixth_low + (square_b * b - b) * sixth_high) * (width * width)
    total = a * value_low + b * value_high + bent
    turn = ((3.0 * square_b - 1.0) * sixth_high - (3.0 * square_a - 1.0) * sixth_low) * width
    slope = (value_high - value_low) * inverse + turn
    return total * scale, slope * scale


def exchange_pairs(group, row):
    far = row < 4
    near = row % 4 < 2
    a, b, c, d = group
    a, c = jnp.where(far, a, pltpu.roll(c, 4, 0)), jnp.where(far, pltpu.roll(a, 4, 0), c)
    b, d = jnp.where(far, b, pltpu.roll(d, 4, 0)), jnp.where(far, pltpu.roll(b, 4, 0), d)
    a, b = jnp.where(near, a, pltpu.roll(b, 2, 0)), jnp.where(near, pltpu.roll(a, 6, 0), b)
    c, d = jnp.where(near, c, pltpu.roll(d, 2, 0)), jnp.where(near, pltpu.roll(c, 6, 0), d)
    return a, b, c, d


def fold_parts(spectra_ref, folded, which, rows, rows_im):
    lanes = slice(which * 128, which * 128 + 128)
    re = [spectra_ref[0, which, s, rows, :].astype(jnp.float32) for s in range(4)]
    im = [spectra_ref[1, which, s, rows, :].astype(jnp.float32) for s in range(4)]
    a_re, b_re, c_re, d_re = re[0] + re[2], re[0] - re[2], re[1] + re[3], re[1] - re[3]
    a_im, b_im, c_im, d_im = im[0] + im[2], im[0] - im[2], im[1] + im[3], im[1] - im[3]
    parts = (
        (a_re + c_re, a_im + c_im),
        (b_re - d_im, b_im + d_re),
        (a_re - c_re, a_im - c_im),
        (b_re + d_im, b_im - d_re),
    )
    for r in range(4):
        folded[r, rows, lanes] = parts[r][0].astype(jnp.bfloat16)
        folded[r, rows_im, lanes] = parts[r][1].astype(jnp.bfloat16)


def push(source, target, send_sem, recv_sem, axis, index):
    return pltpu.make_async_remote_copy(
        src_ref=source,
        dst_ref=target,
        send_sem=send_sem,
        recv_sem=recv_sem,
        device_id={axis: index},
        device_id_type=pl.DeviceIdType.MESH,
    )


def whole_kernel(
    padded,
    mesh_ref,
    spectra_ref,
    table_ref,
    wave_ref,
    density_ref,
    rate_ref,
    gradient_ref,
    out_ref,
    folded,
    comps,
    coef,
    wave_out,
    wave_in,
    sums_out,
    sums_in,
    rim_out,
    rim_in,
    edge_out,
    edge_in,
    first,
    second,
    faces,
    arrived,
    wave_send,
    wave_recv,
    sums_send,
    sums_recv,
    rim_send,
    rim_recv,
    edge_send,
    edge_recv,
    face_send,
    face_recv,
):
    step = pl.program_id(0)
    points = mesh_ref.shape[0]
    quarter_rows = spectra_ref.shape[3]
    depth, height, lanes = density_ref.shape
    per_class = depth // 4
    octets = height // SUB
    blocks = lax.axis_size("gx")
    me = lax.axis_index("gx")
    count = lax.axis_size("yz")
    place = lax.axis_index("yz")
    right, left = lax.rem(place + 1, count), lax.rem(place + count - 1, count)
    after, before = lax.rem(me + 1, blocks), lax.rem(me + blocks - 1, blocks)
    row = lax.broadcasted_iota(jnp.int32, (SUB, lanes), 0)
    lane = lax.broadcasted_iota(jnp.int32, (SUB, lanes), 1)
    edge_copies = [
        push(edge_out.at[0], edge_in.at[0], edge_send.at[0], edge_recv.at[0], "gx", after),
        push(edge_out.at[1], edge_in.at[1], edge_send.at[1], edge_recv.at[1], "gx", before),
    ]

    def to_peer(out, landing, send_sem, recv_sem, peer):
        return push(out.at[peer], landing.at[me], send_sem.at[peer], recv_sem.at[me], "gx", peer)

    def from_peer(out, landing, send_sem, recv_sem, peer):
        return push(out.at[peer], landing.at[peer], send_sem.at[peer], recv_sem.at[peer], "gx", peer)

    waves = (wave_out, wave_in, wave_send, wave_recv)
    sums = (sums_out, sums_in, sums_send, sums_recv)
    rims = (rim_out, rim_in, rim_send, rim_recv)

    @pl.when(step == 0)
    def _():
        barrier = pltpu.get_barrier_semaphore()

        @pl.loop(1, blocks)
        def _(i):
            pl.semaphore_signal(
                barrier, 1, device_id={"gx": lax.rem(me + i, blocks)}, device_id_type=pl.DeviceIdType.MESH
            )

        for neighbour in (left, right):
            pl.semaphore_signal(
                barrier, 1, device_id={"yz": neighbour}, device_id_type=pl.DeviceIdType.MESH
            )
        for octet in range(octets):
            ys = slice(octet * SUB, octet * SUB + SUB)
            for r in range(4):
                for quad in range(padded // SUB):
                    group = [
                        wave_ref[min(4 * (4 * quad + i), depth - 4) + r, ys, :] for i in range(4)
                    ]
                    moved = exchange_pairs(group, row)
                    start = r * padded + quad * SUB
                    for j in range(4):
                        wave_out[4 * octet + j, start : start + SUB, :] = moved[j]
        edge_out[0] = density_ref[depth - 1] * gradient_ref[0, depth - 1]
        edge_out[1] = density_ref[0] * gradient_ref[0, 0]
        pl.semaphore_wait(barrier, blocks + 1)

        @pl.loop(1, blocks)
        def _(i):
            to_peer(*waves, lax.rem(me + i, blocks)).start()

        for copy in edge_copies:
            copy.start()
        wave_in[me] = wave_out[me]

    chunk = 32
    for which in range(2):

        @pl.loop(0, quarter_rows // chunk)
        def _(c):
            rows = pl.ds(pl.multiple_of(c * chunk, chunk), chunk)
            rows_im = pl.ds(pl.multiple_of(c * chunk + quarter_rows, chunk), chunk)
            fold_parts(spectra_ref, folded, which, rows, rows_im)

    for r in range(4):
        product = jnp.dot(table_ref[r], folded[r], preferred_element_type=jnp.float32)
        comps[2 * step, r] = product[:, :128]
        comps[2 * step + 1, r] = product[:, 128:]

    @pl.when(step == pl.num_programs(0) - 1)
    def _():
        spline_coefficients(mesh_ref, coef)
        scale = (quarter_rows * 2) ** (-0.5)

        @pl.loop(1, blocks)
        def _(i):
            from_peer(*waves, lax.rem(me + i, blocks)).wait_recv()

        @pl.loop(1, blocks + 1)
        def _(i):
            block = lax.rem(me + i, blocks)

            @pl.loop(0, 4)
            def _(r):
                for v in range(padded // SUB):
                    source = pl.ds(pl.multiple_of(block * padded + v * SUB, SUB), SUB)
                    low = pl.ds(pl.multiple_of(r * padded + v * SUB, SUB), SUB)
                    high = pl.ds(pl.multiple_of((4 + r) * padded + v * SUB, SUB), SUB)
                    total, slope = spline_sums(
                        wave_in[block, low, :], lambda j: comps[j, r, source, :], coef, points, scale
                    )
                    sums_out[block, low, :] = total
                    sums_out[block, high, :] = slope

            @pl.when(i < blocks)
            def _():
                to_peer(*sums, block).start()

        filled = 2 * per_class
        for block in range(blocks):
            rim_out[block, 0:2, :] = sums_out[
                (block - 1) % blocks, 7 * padded + filled - 2 : 7 * padded + filled, :
            ]
            rim_out[block, 2:4, :] = sums_out[(block + 1) % blocks, 4 * padded : 4 * padded + 2, :]
            rim_out[block, 4:8, :] = jnp.zeros((4, 128), jnp.float32)

        @pl.loop(1, blocks)
        def _(i):
            to_peer(*rims, lax.rem(me + i, blocks)).start()

        sums_in[me] = sums_out[me]
        rim_in[me] = rim_out[me]

        @pl.loop(1, blocks)
        def _(i):
            from_peer(*sums, lax.rem(me + blocks - i, blocks)).wait_recv()

        low_face = [jnp.zeros((SUB, lanes), jnp.float32)] * octets
        high_face = [jnp.zeros((SUB, lanes), jnp.float32)] * octets
        for octet in range(octets):
            ys = slice(octet * SUB, octet * SUB + SUB)
            for r in range(4):
                for quad in range(padded // SUB):
                    low, high = r * padded + quad * SUB, (4 + r) * padded + quad * SUB
                    totals = exchange_pairs(
                        [sums_in[4 * octet + j, low : low + SUB, :] for j in range(4)], row
                    )
                    slopes = exchange_pairs(
                        [sums_in[4 * octet + j, high : high + SUB, :] for j in range(4)], row
                    )
                    for i in range(4):
                        if 4 * quad + i >= per_class:
                            continue
                        x = 4 * (4 * quad + i) + r
                        grad_scale = density_ref[x, ys, :] * slopes[i]
                        third = grad_scale * gradient_ref[2, x, ys, :]
                        onward = jnp.where(lane == lanes - 1, 0.0, pltpu.roll(third, lanes - 1, 1))
                        back = jnp.where(lane == 0, 0.0, pltpu.roll(third, 1, 1))
                        out_ref[x, ys, :] = (
                            totals[i] + rate_ref[x, ys, :] * grad_scale - 0.5 * (onward - back)
                        )
                        first[x + 1, ys, :] = grad_scale * gradient_ref[0, x, ys, :]
                        second[x, ys, :] = grad_scale * gradient_ref[1, x, ys, :]
                        low_face[octet] = jnp.where(lane == x, third[:, :1], low_face[octet])
                        high_face[octet] = jnp.where(lane == x, third[:, lanes - 1 :], high_face[octet])
            faces[0, ys, :] = low_face[octet]
            faces[1, ys, :] = high_face[octet]

        face_copies = [
            push(faces.at[side], arrived.at[side], face_send.at[side], face_recv.at[side], "yz", neighbour)
            for side, neighbour in ((0, left), (1, right))
        ]
        for copy in face_copies:
            copy.start()

        @pl.loop(1, blocks)
        def _(i):
            from_peer(*rims, lax.rem(me + i, blocks)).wait_recv()

        for copy in edge_copies:
            copy.wait()
        for octet in range(octets):
            ys = slice(octet * SUB, octet * SUB + SUB)
            for side, x in ((0, 0), (1, depth + 1)):
                edge = jnp.zeros((SUB, lanes), jnp.float32)
                for j in range(4):
                    piece = rim_in[4 * octet + j]
                    shift = (2 * j - 2 * side) % SUB
                    piece = pltpu.roll(piece, shift, 0) if shift else piece
                    edge = jnp.where(row // 2 == j, piece, edge)
                first[x, ys, :] = edge * edge_in[side, ys, :]

        @pl.loop(0, depth)
        def _(x):
            pieces = [second[x, o * SUB : o * SUB + SUB, :] for o in range(octets)]
            up = [pltpu.roll(p, SUB - 1, 0) for p in pieces]
            down = [pltpu.roll(p, 1, 0) for p in pieces]
            for o in range(octets):
                ys = slice(o * SUB, o * SUB + SUB)
                following = jnp.where(row == SUB - 1, up[(o + 1) % octets], up[o])
                previous = jnp.where(row == 0, down[o - 1], down[o])
                along = first[x + 2, ys, :] - first[x, ys, :]
                out_ref[x, ys, :] = out_ref[x, ys, :] - 0.5 * (along + (following - previous))

        for copy in face_copies:
            copy.wait()
        for o in range(octets):
            ys = slice(o * SUB, o * SUB + SUB)
            next_face, previous_face = arrived[0, ys, :], arrived[1, ys, :]
            for x in range(depth):
                edges = jnp.where(lane == lanes - 1, next_face[:, x : x + 1], 0.0) - jnp.where(
                    lane == 0, previous_face[:, x : x + 1], 0.0
                )
                out_ref[x, ys, :] = out_ref[x, ys, :] - 0.5 * edges

        @pl.loop(1, blocks)
        def _(i):
            peer = lax.rem(me + i, blocks)
            to_peer(*waves, peer).wait_send()
            to_peer(*sums, peer).wait_send()
            to_peer(*rims, peer).wait_send()


def solution(mesh):
    blocks = mesh.shape["gx"]

    def shards(spectra, kernel_mesh, density, local_wave, wave_density, wave_gradient):
        _, points, length, thin, lanes = spectra.shape
        depth, height, _ = density.shape
        padded = -(-2 * (depth // 4) // SUB) * SUB
        rows = length // 4 * thin
        table = jnp.asarray(split_tables(length, blocks, padded))
        spectra = spectra.reshape(2, points, 4, rows, lanes)

        def fixed(array):
            zeros = (0,) * array.ndim
            return pl.BlockSpec(array.shape, lambda i: zeros)

        def real(*shape):
            return pltpu.VMEM(shape, jnp.float32)

        many = pltpu.SemaphoreType.DMA((blocks,))
        pair = pltpu.SemaphoreType.DMA((2,))
        return pl.pallas_call(
            functools.partial(whole_kernel, padded),
            grid=(points // 2,),
            out_shape=jax.ShapeDtypeStruct(density.shape, jnp.float32),
            in_specs=[
                pl.BlockSpec(memory_space=pltpu.SMEM),
                pl.BlockSpec((2, 2, 4, rows, lanes), lambda i: (0, i, 0, 0, 0)),
                fixed(table),
                fixed(local_wave),
                fixed(density),
                fixed(wave_density),
                fixed(wave_gradient),
            ],
            out_specs=fixed(density),
            scratch_shapes=[
                pltpu.VMEM((4, 2 * rows, 2 * lanes), jnp.bfloat16),
                real(points, 4, blocks * padded, lanes),
                real(5, points, SUB, lanes),
                real(blocks, 4 * padded, lanes),
                real(blocks, 4 * padded, lanes),
                real(blocks, 8 * padded, lanes),
                real(blocks, 8 * padded, lanes),
                real(blocks, SUB, lanes),
                real(blocks, SUB, lanes),
                real(2, height, lanes),
                real(2, height, lanes),
                real(depth + 2, height, lanes),
                real(depth, height, lanes),
                real(2, height, lanes),
                real(2, height, lanes),
            ]
            + [many] * 6
            + [pair] * 4,
            compiler_params=pltpu.CompilerParams(
                collective_id=0,
                has_side_effects=True,
                dimension_semantics=("arbitrary",),
                vmem_limit_bytes=60 * 1024 * 1024,
            ),
        )(kernel_mesh, spectra, table, local_wave, density, wave_density, wave_gradient)

    return jax.shard_map(
        shards,
        mesh=mesh,
        in_specs=(
            P(None, None, None, "gx", "yz"),
            P(),
            P("gx", None, "yz"),
            P("gx", None, "yz"),
            P("gx", None, "yz"),
            P(None, "gx", None, "yz"),
        ),
        out_specs=P("gx", None, "yz"),
        check_vma=False,
    )
```

```python
import functools
import math

import jax
import jax.numpy as jnp
import numpy as np
from jax import lax
from jax.experimental import pallas as pl
from jax.experimental.pallas import tpu as pltpu
from jax.sharding import PartitionSpec as P

SUB = 8


def split_tables(length, blocks, padded_rows):
    quarter = length // 4
    per_block = length // blocks // 4
    out = np.zeros((4, blocks, padded_rows, 2, quarter, 2), np.float32)
    k = np.arange(quarter)
    for r in range(4):
        m = np.arange(blocks * per_block).reshape(blocks, per_block)
        x = 4 * m + r
        phases = (x[..., None] * k) % length
        angles = phases.astype(np.float32) * np.float32(2.0 * math.pi / length)
        pair = np.stack([np.cos(angles), -np.sin(angles)], axis=2)
        for y in range(2):
            out[r, :, y : 2 * per_block : 2, :, :, y] = pair
    flat = out.reshape(4, blocks * padded_rows, 4 * quarter)
    return flat.astype(jnp.bfloat16)


def spline_coefficients(mesh_ref, coef_ref):
    points = mesh_ref.shape[0]
    ones = jnp.ones((SUB, 128), jnp.float32)
    node = [ones * mesh_ref[j] for j in range(points)]
    gap = [node[j + 1] - node[j] for j in range(points - 1)]
    carry = jnp.zeros((SUB, 128), jnp.float32)
    for j in range(points):
        coef_ref[0, j] = node[j]
        if j < points - 1:
            coef_ref[1, j] = 1.0 / gap[j]
        if 1 <= j < points - 1:
            pivot = 1.0 / (2.0 * (gap[j - 1] + gap[j]) - gap[j - 1] * carry)
            carry = gap[j] * pivot
            coef_ref[2, j] = pivot
            coef_ref[3, j] = gap[j - 1] * pivot
            coef_ref[4, j] = carry


def spline_sums(wave, value_of, coef_ref, points, scale):
    values = [value_of(j) for j in range(points)]
    forward = [None] * points
    slope_before = (values[1] - values[0]) * coef_ref[1, 0]
    for j in range(1, points - 1):
        slope_here = (values[j + 1] - values[j]) * coef_ref[1, j]
        term = (slope_here - slope_before) * coef_ref[2, j]
        if j > 1:
            term = term - coef_ref[3, j] * forward[j - 1]
        forward[j] = term
        slope_before = slope_here
    zero = jnp.zeros_like(wave)
    sixth = [zero] * points
    for j in range(points - 2, 0, -1):
        sixth[j] = forward[j] if j == points - 2 else forward[j] - coef_ref[4, j] * sixth[j + 1]
    picked = [values[0], values[1], sixth[0], sixth[1], coef_ref[0, 0], coef_ref[0, 1]]
    for j in range(1, points - 1):
        above = wave >= coef_ref[0, j]
        here = [values[j], values[j + 1], sixth[j], sixth[j + 1], coef_ref[0, j], coef_ref[0, j + 1]]
        picked = [jnp.where(above, new, old) for new, old in zip(here, picked)]
    value_low, value_high, sixth_low, sixth_high, low, high = picked
    width = high - low
    inverse = 1.0 / width
    a = (high - wave) * inverse
    b = (wave - low) * inverse
    square_a, square_b = a * a, b * b
    bent = ((square_a * a - a) * sixth_low + (square_b * b - b) * sixth_high) * (width * width)
    total = a * value_low + b * value_high + bent
    turn = ((3.0 * square_b - 1.0) * sixth_high - (3.0 * square_a - 1.0) * sixth_low) * width
    slope = (value_high - value_low) * inverse + turn
    return total * scale, slope * scale


def exchange_pairs(group, row):
    far = row < 4
    near = row % 4 < 2
    a, b, c, d = group
    a, c = jnp.where(far, a, pltpu.roll(c, 4, 0)), jnp.where(far, pltpu.roll(a, 4, 0), c)
    b, d = jnp.where(far, b, pltpu.roll(d, 4, 0)), jnp.where(far, pltpu.roll(b, 4, 0), d)
    a, b = jnp.where(near, a, pltpu.roll(b, 2, 0)), jnp.where(near, pltpu.roll(a, 6, 0), b)
    c, d = jnp.where(near, c, pltpu.roll(d, 2, 0)), jnp.where(near, pltpu.roll(c, 6, 0), d)
    return a, b, c, d


def fold_parts(spectra_ref, folded, which, rows, rows_im):
    lanes = slice(which * 128, which * 128 + 128)
    re = [spectra_ref[0, which, s, rows, :].astype(jnp.float32) for s in range(4)]
    im = [spectra_ref[1, which, s, rows, :].astype(jnp.float32) for s in range(4)]
    a_re, b_re, c_re, d_re = re[0] + re[2], re[0] - re[2], re[1] + re[3], re[1] - re[3]
    a_im, b_im, c_im, d_im = im[0] + im[2], im[0] - im[2], im[1] + im[3], im[1] - im[3]
    parts = (
        (a_re + c_re, a_im + c_im),
        (b_re - d_im, b_im + d_re),
        (a_re - c_re, a_im - c_im),
        (b_re + d_im, b_im - d_re),
    )
    for r in range(4):
        folded[r, rows, lanes] = parts[r][0].astype(jnp.bfloat16)
        folded[r, rows_im, lanes] = parts[r][1].astype(jnp.bfloat16)


def push(source, target, send_sem, recv_sem, axis, index):
    return pltpu.make_async_remote_copy(
        src_ref=source,
        dst_ref=target,
        send_sem=send_sem,
        recv_sem=recv_sem,
        device_id={axis: index},
        device_id_type=pl.DeviceIdType.MESH,
    )


def peer_order(blocks):
    masks = sorted(range(1, blocks), key=lambda m: (-bin(m // 2).count("1"), m % 2, m))
    return masks + [0]


def peer_at(me, blocks, i):
    if blocks & (blocks - 1):
        return lax.rem(me + i, blocks)
    mask = 0
    for turn, value in enumerate(peer_order(blocks)):
        mask = mask + jnp.where(i == turn + 1, value, 0)
    peer = me
    bit = 1
    while bit < blocks:
        peer = peer + ((mask // bit) % 2) * bit * (1 - 2 * ((me // bit) % 2))
        bit *= 2
    return peer


def whole_kernel(
    padded,
    mesh_ref,
    spectra_ref,
    table_ref,
    wave_ref,
    density_ref,
    rate_ref,
    gradient_ref,
    out_ref,
    folded,
    comps,
    coef,
    wave_out,
    wave_in,
    sums_out,
    sums_in,
    rim_out,
    rim_in,
    edge_out,
    edge_in,
    first,
    second,
    faces,
    arrived,
    wave_send,
    wave_recv,
    sums_send,
    sums_recv,
    rim_send,
    rim_recv,
    edge_send,
    edge_recv,
    face_send,
    face_recv,
):
    step = pl.program_id(0)
    points = mesh_ref.shape[0]
    quarter_rows = spectra_ref.shape[3]
    depth, height, lanes = density_ref.shape
    per_class = depth // 4
    octets = height // SUB
    blocks = lax.axis_size("gx")
    me = lax.axis_index("gx")
    count = lax.axis_size("yz")
    place = lax.axis_index("yz")
    right, left = lax.rem(place + 1, count), lax.rem(place + count - 1, count)
    after, before = lax.rem(me + 1, blocks), lax.rem(me + blocks - 1, blocks)
    row = lax.broadcasted_iota(jnp.int32, (SUB, lanes), 0)
    lane = lax.broadcasted_iota(jnp.int32, (SUB, lanes), 1)
    edge_copies = [
        push(edge_out.at[0], edge_in.at[0], edge_send.at[0], edge_recv.at[0], "gx", after),
        push(edge_out.at[1], edge_in.at[1], edge_send.at[1], edge_recv.at[1], "gx", before),
    ]

    def to_peer(out, landing, send_sem, recv_sem, peer):
        return push(out.at[peer], landing.at[me], send_sem.at[peer], recv_sem.at[me], "gx", peer)

    def from_peer(out, landing, send_sem, recv_sem, peer):
        return push(out.at[peer], landing.at[peer], send_sem.at[peer], recv_sem.at[peer], "gx", peer)

    waves = (wave_out, wave_in, wave_send, wave_recv)
    sums = (sums_out, sums_in, sums_send, sums_recv)
    rims = (rim_out, rim_in, rim_send, rim_recv)

    @pl.when(step == 0)
    def _():
        barrier = pltpu.get_barrier_semaphore()

        @pl.loop(1, blocks)
        def _(i):
            pl.semaphore_signal(
                barrier, 1, device_id={"gx": lax.rem(me + i, blocks)}, device_id_type=pl.DeviceIdType.MESH
            )

        for neighbour in (left, right):
            pl.semaphore_signal(
                barrier, 1, device_id={"yz": neighbour}, device_id_type=pl.DeviceIdType.MESH
            )
        for octet in range(octets):
            ys = slice(octet * SUB, octet * SUB + SUB)
            for r in range(4):
                for quad in range(padded // SUB):
                    group = [
                        wave_ref[min(4 * (4 * quad + i), depth - 4) + r, ys, :] for i in range(4)
                    ]
                    moved = exchange_pairs(group, row)
                    start = r * padded + quad * SUB
                    for j in range(4):
                        wave_out[4 * octet + j, start : start + SUB, :] = moved[j]
        edge_out[0] = density_ref[depth - 1] * gradient_ref[0, depth - 1]
        edge_out[1] = density_ref[0] * gradient_ref[0, 0]
        pl.semaphore_wait(barrier, blocks + 1)

        @pl.loop(1, blocks)
        def _(i):
            to_peer(*waves, peer_at(me, blocks, i)).start()

        for copy in edge_copies:
            copy.start()
        wave_in[me] = wave_out[me]

    chunk = 32
    for which in range(2):

        @pl.loop(0, quarter_rows // chunk)
        def _(c):
            rows = pl.ds(pl.multiple_of(c * chunk, chunk), chunk)
            rows_im = pl.ds(pl.multiple_of(c * chunk + quarter_rows, chunk), chunk)
            fold_parts(spectra_ref, folded, which, rows, rows_im)

    for r in range(4):
        product = jnp.dot(table_ref[r], folded[r], preferred_element_type=jnp.float32)
        comps[2 * step, r] = product[:, :128]
        comps[2 * step + 1, r] = product[:, 128:]

    @pl.when(step == pl.num_programs(0) - 1)
    def _():
        spline_coefficients(mesh_ref, coef)
        scale = (quarter_rows * 2) ** (-0.5)

        @pl.loop(1, blocks)
        def _(i):
            from_peer(*waves, lax.rem(me + i, blocks)).wait_recv()

        @pl.loop(1, blocks + 1)
        def _(i):
            block = peer_at(me, blocks, i)

            @pl.loop(0, 4)
            def _(r):
                for v in range(padded // SUB):
                    source = pl.ds(pl.multiple_of(block * padded + v * SUB, SUB), SUB)
                    low = pl.ds(pl.multiple_of(r * padded + v * SUB, SUB), SUB)
                    high = pl.ds(pl.multiple_of((4 + r) * padded + v * SUB, SUB), SUB)
                    total, slope = spline_sums(
                        wave_in[block, low, :], lambda j: comps[j, r, source, :], coef, points, scale
                    )
                    sums_out[block, low, :] = total
                    sums_out[block, high, :] = slope

            @pl.when(i < blocks)
            def _():
                to_peer(*sums, block).start()

        filled = 2 * per_class
        for block in range(blocks):
            rim_out[block, 0:2, :] = sums_out[
                (block - 1) % blocks, 7 * padded + filled - 2 : 7 * padded + filled, :
            ]
            rim_out[block, 2:4, :] = sums_out[(block + 1) % blocks, 4 * padded : 4 * padded + 2, :]
            rim_out[block, 4:8, :] = jnp.zeros((4, 128), jnp.float32)

        @pl.loop(1, blocks)
        def _(i):
            to_peer(*rims, lax.rem(me + i, blocks)).start()

        sums_in[me] = sums_out[me]
        rim_in[me] = rim_out[me]

        @pl.loop(1, blocks)
        def _(i):
            from_peer(*sums, lax.rem(me + blocks - i, blocks)).wait_recv()

        low_face = [jnp.zeros((SUB, lanes), jnp.float32)] * octets
        high_face = [jnp.zeros((SUB, lanes), jnp.float32)] * octets
        for octet in range(octets):
            ys = slice(octet * SUB, octet * SUB + SUB)
            for r in range(4):
                for quad in range(padded // SUB):
                    low, high = r * padded + quad * SUB, (4 + r) * padded + quad * SUB
                    totals = exchange_pairs(
                        [sums_in[4 * octet + j, low : low + SUB, :] for j in range(4)], row
                    )
                    slopes = exchange_pairs(
                        [sums_in[4 * octet + j, high : high + SUB, :] for j in range(4)], row
                    )
                    for i in range(4):
                        if 4 * quad + i >= per_class:
                            continue
                        x = 4 * (4 * quad + i) + r
                        grad_scale = density_ref[x, ys, :] * slopes[i]
                        third = grad_scale * gradient_ref[2, x, ys, :]
                        onward = jnp.where(lane == lanes - 1, 0.0, pltpu.roll(third, lanes - 1, 1))
                        back = jnp.where(lane == 0, 0.0, pltpu.roll(third, 1, 1))
                        out_ref[x, ys, :] = (
                            totals[i] + rate_ref[x, ys, :] * grad_scale - 0.5 * (onward - back)
                        )
                        first[x + 1, ys, :] = grad_scale * gradient_ref[0, x, ys, :]
                        second[x, ys, :] = grad_scale * gradient_ref[1, x, ys, :]
                        low_face[octet] = jnp.where(lane == x, third[:, :1], low_face[octet])
                        high_face[octet] = jnp.where(lane == x, third[:, lanes - 1 :], high_face[octet])
            faces[0, ys, :] = low_face[octet]
            faces[1, ys, :] = high_face[octet]

        face_copies = [
            push(faces.at[side], arrived.at[side], face_send.at[side], face_recv.at[side], "yz", neighbour)
            for side, neighbour in ((0, left), (1, right))
        ]
        for copy in face_copies:
            copy.start()

        @pl.loop(1, blocks)
        def _(i):
            from_peer(*rims, lax.rem(me + i, blocks)).wait_recv()

        for copy in edge_copies:
            copy.wait()
        for octet in range(octets):
            ys = slice(octet * SUB, octet * SUB + SUB)
            for side, x in ((0, 0), (1, depth + 1)):
                edge = jnp.zeros((SUB, lanes), jnp.float32)
                for j in range(4):
                    piece = rim_in[4 * octet + j]
                    shift = (2 * j - 2 * side) % SUB
                    piece = pltpu.roll(piece, shift, 0) if shift else piece
                    edge = jnp.where(row // 2 == j, piece, edge)
                first[x, ys, :] = edge * edge_in[side, ys, :]

        @pl.loop(0, depth)
        def _(x):
            pieces = [second[x, o * SUB : o * SUB + SUB, :] for o in range(octets)]
            up = [pltpu.roll(p, SUB - 1, 0) for p in pieces]
            down = [pltpu.roll(p, 1, 0) for p in pieces]
            for o in range(octets):
                ys = slice(o * SUB, o * SUB + SUB)
                following = jnp.where(row == SUB - 1, up[(o + 1) % octets], up[o])
                previous = jnp.where(row == 0, down[o - 1], down[o])
                along = first[x + 2, ys, :] - first[x, ys, :]
                out_ref[x, ys, :] = out_ref[x, ys, :] - 0.5 * (along + (following - previous))

        for copy in face_copies:
            copy.wait()
        for o in range(octets):
            ys = slice(o * SUB, o * SUB + SUB)
            next_face, previous_face = arrived[0, ys, :], arrived[1, ys, :]
            for x in range(depth):
                edges = jnp.where(lane == lanes - 1, next_face[:, x : x + 1], 0.0) - jnp.where(
                    lane == 0, previous_face[:, x : x + 1], 0.0
                )
                out_ref[x, ys, :] = out_ref[x, ys, :] - 0.5 * edges

        @pl.loop(1, blocks)
        def _(i):
            peer = lax.rem(me + i, blocks)
            to_peer(*waves, peer).wait_send()
            to_peer(*sums, peer).wait_send()
            to_peer(*rims, peer).wait_send()


def solution(mesh):
    blocks = mesh.shape["gx"]

    def shards(spectra, kernel_mesh, density, local_wave, wave_density, wave_gradient):
        _, points, length, thin, lanes = spectra.shape
        depth, height, _ = density.shape
        padded = -(-2 * (depth // 4) // SUB) * SUB
        rows = length // 4 * thin
        table = jnp.asarray(split_tables(length, blocks, padded))
        spectra = spectra.reshape(2, points, 4, rows, lanes)

        def fixed(array):
            zeros = (0,) * array.ndim
            return pl.BlockSpec(array.shape, lambda i: zeros)

        def real(*shape):
            return pltpu.VMEM(shape, jnp.float32)

        many = pltpu.SemaphoreType.DMA((blocks,))
        pair = pltpu.SemaphoreType.DMA((2,))
        return pl.pallas_call(
            functools.partial(whole_kernel, padded),
            grid=(points // 2,),
            out_shape=jax.ShapeDtypeStruct(density.shape, jnp.float32),
            in_specs=[
                pl.BlockSpec(memory_space=pltpu.SMEM),
                pl.BlockSpec((2, 2, 4, rows, lanes), lambda i: (0, i, 0, 0, 0)),
                fixed(table),
                fixed(local_wave),
                fixed(density),
                fixed(wave_density),
                fixed(wave_gradient),
            ],
            out_specs=fixed(density),
            scratch_shapes=[
                pltpu.VMEM((4, 2 * rows, 2 * lanes), jnp.bfloat16),
                real(points, 4, blocks * padded, lanes),
                real(5, points, SUB, lanes),
                real(blocks, 4 * padded, lanes),
                real(blocks, 4 * padded, lanes),
                real(blocks, 8 * padded, lanes),
                real(blocks, 8 * padded, lanes),
                real(blocks, SUB, lanes),
                real(blocks, SUB, lanes),
                real(2, height, lanes),
                real(2, height, lanes),
                real(depth + 2, height, lanes),
                real(depth, height, lanes),
                real(2, height, lanes),
                real(2, height, lanes),
            ]
            + [many] * 6
            + [pair] * 4,
            compiler_params=pltpu.CompilerParams(
                collective_id=0,
                has_side_effects=True,
                dimension_semantics=("arbitrary",),
                vmem_limit_bytes=60 * 1024 * 1024,
            ),
        )(kernel_mesh, spectra, table, local_wave, density, wave_density, wave_gradient)

    return jax.shard_map(
        shards,
        mesh=mesh,
        in_specs=(
            P(None, None, None, "gx", "yz"),
            P(),
            P("gx", None, "yz"),
            P("gx", None, "yz"),
            P("gx", None, "yz"),
            P(None, "gx", None, "yz"),
        ),
        out_specs=P("gx", None, "yz"),
        check_vma=False,
    )
```
